256 devices in a mesh: south: 4 (over x), east: 4 (over y), down: 16 (over z, core).
Axes of the slice: x: 4, y: 4, z: 8, core: 2. Of those that a mesh axis runs over, the one named last changes fastest.
Arguments:
- field_values: float32 [32, 384, 128, 128], P('south', 'east', 'down'), may hold values from 0.2 to 1.8
- flow_y: float32 [32, 384, 128, 128], P('south', 'east', 'down'), may hold values from -0.3 to 0.3
- flow_x: float32 [32, 384, 128, 128], P('south', 'east', 'down'), may hold values from -0.3 to 0.3
- flow_z: float32 [32, 384, 128, 128], P('south', 'east', 'down'), may hold values from -0.3 to 0.3
Outputs:
- potential: float32 [32, 384, 128, 128], P('south', 'east', 'down')
- field_values_end: float32 [32, 384, 128, 128], P('south', 'east', 'down')
The draws below stay inside these ranges and needn't reach their ends.
All inputs are finite; a program needn't handle non-finite values.
Results may differ from the reference program's by a relative error of at most 0.00002.
Values sent between devices are 32-bit elements; how exact they have to be, the bound alone decides.
No kernel may reach another device: no remote copies, remote signals or barrier semaphores. Data moves between devices by JAX's collectives and lax.ppermute only.
A program may use at most 128 MiB of HBM per device.

```python
import jax
import jax.numpy as jnp
from jax import lax

GRID_Y = 32
GRID_X = 384
GRID_Z = 128
LEVELS = 128
STEPS = 4


def level_of(own_key, extent, cuts, low, largest):
    factor_of = 1.0
    for position, parts in cuts:
        steps = jax.random.uniform(jax.random.fold_in(jax.random.fold_in(own_key, 6), position), (parts,), jnp.float32, low / len(cuts), largest / len(cuts))
        factor_of = factor_of * jnp.repeat(jnp.exp(steps), extent[position] // parts).reshape((-1,) + (1,) * (len(extent) - 1 - position))
    return factor_of


def setup_inputs(seed: int = 0) -> dict:
    seeds = jax.random.split(jax.random.key(seed), 5)
    field_values = jnp.clip(0.2 + 1.5999999 * jax.random.uniform(seeds[0], (GRID_Y, GRID_X, GRID_Z, LEVELS), jnp.float32) ** level_of(seeds[0], (GRID_Y, GRID_X, GRID_Z, LEVELS), ((0, 4), (1, 4), (2, 16)), -0.2, 0.2), 0.2, 1.8)
    flow_y = jnp.clip(jax.random.uniform(seeds[1], (GRID_Y, GRID_X, GRID_Z, LEVELS), jnp.float32, -0.3, 0.3) * level_of(seeds[1], (GRID_Y, GRID_X, GRID_Z, LEVELS), ((0, 4), (1, 4), (2, 16)), -0.4, 0.0), -0.3, 0.3)
    flow_x = jnp.clip(jax.random.uniform(seeds[2], (GRID_Y, GRID_X, GRID_Z, LEVELS), jnp.float32, -0.3, 0.3) * level_of(seeds[2], (GRID_Y, GRID_X, GRID_Z, LEVELS), ((0, 4), (1, 4), (2, 16)), -0.4, 0.0), -0.3, 0.3)
    flow_z = jnp.clip(jax.random.uniform(seeds[3], (GRID_Y, GRID_X, GRID_Z, LEVELS), jnp.float32, -0.3, 0.3) * level_of(seeds[3], (GRID_Y, GRID_X, GRID_Z, LEVELS), ((0, 4), (1, 4), (2, 16)), -0.4, 0.0), -0.3, 0.3)
    return {"field_values": field_values, "flow_y": flow_y, "flow_x": flow_x, "flow_z": flow_z}


def without_rim(values, dims):
    for dim in dims:
        values = lax.slice_in_dim(values, 1, values.shape[dim] - 1, axis=dim)
    return values


def shifted_cells(values, dim, start, dims):
    others = [other for other in dims if other != dim]
    values = without_rim(values, others)
    return lax.slice_in_dim(values, start, start + values.shape[dim] - 2, axis=dim)


def march_step(padded, flow_y, flow_x, flow_z):
    middle = without_rim(padded, (0, 1, 2))
    lower = [shifted_cells(padded, dim, 0, (0, 1, 2)) for dim in (0, 1, 2)]
    upper = [shifted_cells(padded, dim, 2, (0, 1, 2)) for dim in (0, 1, 2)]
    slopes = [above - below for above, below in zip(upper, lower)]
    smooth_rate = 0.05
    spread = lower[0] + upper[0] + lower[1] + upper[1] + lower[2] + upper[2] - 6.0 * middle
    return middle - flow_y * slopes[0] - flow_x * slopes[1] - flow_z * slopes[2] + smooth_rate * spread


def reference(field_values, flow_y, flow_x, flow_z):
    for step in range(STEPS):
        field_values = march_step(jnp.pad(field_values, ((1, 1), (1, 1), (1, 1), (0, 0)), mode="wrap"), flow_y, flow_x, flow_z)
    potential = jnp.cumsum(field_values, axis=2) / GRID_Z
    return potential, field_values
```

```python
import functools

import jax
import jax.numpy as jnp
from jax import lax
from jax.experimental import pallas as pl
from jax.experimental.pallas import tpu as pltpu
from jax.sharding import Mesh
from jax.sharding import PartitionSpec as P

STEPS = 4
RATE = 0.05
BLOCK = 8
VMEM = 5 << 20


DOWN = ("chip", "core")
IN_VMEM = pl.BlockSpec(memory_space=pltpu.VMEM)
IN_HBM = pl.BlockSpec(memory_space=pltpu.HBM)


def shape(*dims):
    return jax.ShapeDtypeStruct(dims, jnp.float32)


def call(kernel, outs, *args, flops=1 << 21, in_specs=None, out_specs=None, scratch=(), alias=None):
    return pl.pallas_call(
        kernel,
        out_shape=outs,
        in_specs=in_specs or [IN_VMEM] * len(args),
        out_specs=out_specs or [IN_VMEM] * len(outs),
        scratch_shapes=scratch,
        input_output_aliases=alias or {},
        compiler_params=pltpu.CompilerParams(vmem_limit_bytes=VMEM),
        cost_estimate=pl.CostEstimate(flops=flops, bytes_accessed=0, transcendentals=0),
    )(*args)


def march_row(row, cells, here, above, below, put, downs, flows, sides=None):
    zlo, zhi = downs
    fy, fx, fz = flows
    sublane = lax.broadcasted_iota(jnp.int32, (8, 128), 0)

    def cell(x, left, mid, right):
        up, down = above(x), below(x)
        head = jnp.broadcast_to(zhi[row, pl.ds(x, 1), :], (8, 128))
        tail = jnp.broadcast_to(zlo[row, pl.ds(x, 1), :], (8, 128))
        ahead = jnp.where(sublane == 7, head, pltpu.roll(mid, 7, 0))
        behind = jnp.where(sublane == 0, tail, pltpu.roll(mid, 1, 0))
        around = ((up + down) + (left + right)) + (ahead + behind)
        carried = (fy[row, x] * (up - down) + fx[row, x] * (right - left)) + fz[row, x] * (ahead - behind)
        put(x, ((1.0 - 6.0 * RATE) * mid + RATE * around) - carried)

    def run(start, count, left, mid):
        for k in range(count):
            right = here(start + k + 1)
            cell(start + k, left, mid, right)
            left, mid = mid, right
        return left, mid

    def body(i, carry):
        return run(pl.multiple_of(i * BLOCK, BLOCK), BLOCK, *carry)

    if sides is not None:
        cell(0, sides[0][row], here(0), here(1))
        cell(cells - 1, here(cells - 2), here(cells - 1), sides[1][row])
    carry = run(1, BLOCK - 1, here(0), here(1))
    carry = lax.fori_loop(1, cells // BLOCK - 1, body, carry)
    run(cells - BLOCK, BLOCK - 1, *carry)


def march_sides(row, cells, here, above, below, put, downs, flows, sides):
    zlo, zhi = downs
    fy, fx, fz = flows
    sublane = lax.broadcasted_iota(jnp.int32, (8, 128), 0)
    for x, left, right in ((0, sides[0][row], here(1)), (cells - 1, here(cells - 2), sides[1][row])):
        mid, up, down = here(x), above(x), below(x)
        head = jnp.broadcast_to(zhi[row, pl.ds(x, 1), :], (8, 128))
        tail = jnp.broadcast_to(zlo[row, pl.ds(x, 1), :], (8, 128))
        ahead = jnp.where(sublane == 7, head, pltpu.roll(mid, 7, 0))
        behind = jnp.where(sublane == 0, tail, pltpu.roll(mid, 1, 0))
        around = ((up + down) + (left + right)) + (ahead + behind)
        carried = (fy[row, x] * (up - down) + fx[row, x] * (right - left)) + fz[row, x] * (ahead - behind)
        put(x, ((1.0 - 6.0 * RATE) * mid + RATE * around) - carried)


def reader(ref, *at):
    return lambda x: ref[(*at, x)]


def writer(ref, *at):
    def put(x, value):
        ref[(*at, x)] = value

    return put


def planes_of(refs, height):
    if len(refs) == 1:
        return [refs[0].at[y] for y in range(height)]
    low, inner, high = refs
    return [low, *(inner.at[y] for y in range(height - 2)), high]


def inner_kernel(parts, height, *refs):
    field, downs, flows, (out,) = refs[:parts], refs[parts : parts + 2], refs[parts + 2 : parts + 5], refs[parts + 5 :]
    rows = [reader(plane) for plane in planes_of(field, height)]
    for y in range(1, height - 1):
        march_row(y, flows[0].shape[1], rows[y], rows[y + 1], rows[y - 1], writer(out, y - 1), downs, flows)


def rim_kernel(parts, height, *refs):
    field, downs, flows = refs[:parts], refs[parts : parts + 2], refs[parts + 2 : parts + 5]
    sides, (slo, shi) = refs[parts + 5 : parts + 7], refs[parts + 7 : parts + 9]
    mid, low, high = refs[parts + 10 :]
    cells = flows[0].shape[1]
    rows = [reader(plane) for plane in planes_of(field, height)]
    puts = [writer(low), *(writer(mid, y) for y in range(height - 2)), writer(high)]
    for y in range(height):
        above = reader(shi) if y == height - 1 else rows[y + 1]
        below = reader(slo) if y == 0 else rows[y - 1]
        march = march_row if y in (0, height - 1) else march_sides
        march(y, cells, rows[y], above, below, puts[y], downs, flows, sides)


def rows_kernel(field, low, high, done):
    copies = [
        pltpu.make_async_copy(field.at[0], low, done.at[0]),
        pltpu.make_async_copy(field.at[field.shape[0] - 1], high, done.at[1]),
    ]
    for copy in copies:
        copy.start()
    for copy in copies:
        copy.wait()


def faces_kernel(parts, height, *refs):
    field, (first, last, left, right) = refs[:parts], refs[parts:]
    cells = first.shape[1]
    for y, plane in enumerate(planes_of(field, height)):
        flat = plane.reshape(cells * 8, 128)
        first[y] = flat[pl.ds(0, cells, 8), :]
        last[y] = flat[pl.ds(7, cells, 8), :]
        left[y] = plane[0]
        right[y] = plane[cells - 1]


def totals_kernel(core, low, inner, high, own, other, end, done):
    half, cells = own.shape[:2]
    planes = planes_of((low, inner, high), 2 * half)
    copies = [
        pltpu.make_async_copy(low, end.at[0], done.at[0]),
        pltpu.make_async_copy(inner, end.at[pl.ds(1, 2 * half - 2)], done.at[1]),
        pltpu.make_async_copy(high, end.at[2 * half - 1], done.at[2]),
    ]
    for copy in copies:
        copy.start()

    def add_up(out, planes):
        for y, plane in enumerate(planes):
            flat = plane.reshape(cells * 8, 128)
            terms = [flat[pl.ds(k, cells, 8), :] for k in range(8)]
            out[y] = ((terms[0] + terms[1]) + (terms[2] + terms[3])) + ((terms[4] + terms[5]) + (terms[6] + terms[7]))

    @pl.when(core[0] == 0)
    def _():
        add_up(own, planes[:half])
        add_up(other, planes[half:])

    @pl.when(core[0] != 0)
    def _():
        add_up(own, planes[half:])
        add_up(other, planes[:half])

    for copy in copies:
        copy.wait()


def add_kernel(a, b, out):
    out[...] = a[...] + b[...]


def before_kernel(pieces, out):
    so_far = jnp.zeros(pieces.shape[1:], jnp.float32)
    for k in range(pieces.shape[0]):
        out[k] = so_far
        so_far = so_far + pieces[k]


def split_kernel(core, chips, own, got, mine, partners):
    @pl.when(core[0] == 0)
    def _():
        mine[...] = chips[...]
        partners[...] = chips[...] + own[...]

    @pl.when(core[0] != 0)
    def _():
        mine[...] = chips[...] + got[...]
        partners[...] = chips[...]


def potential_kernel(scale, core, low, inner, high, mine, theirs, out, held, done):
    half, cells = mine.shape[:2]
    sublane = lax.broadcasted_iota(jnp.int32, (8, 128), 0)
    planes = planes_of((low, inner, high), 2 * half)

    def fill(y, before, j):
        def body(i, carry):
            start = pl.multiple_of(i * BLOCK, BLOCK)
            for k in range(BLOCK):
                x = start + k
                value = planes[y][x]
                for reach in (1, 2, 4):
                    value = value + jnp.where(sublane >= reach, pltpu.roll(value, reach, 0), 0.0)
                held[y, x] = (value + jnp.broadcast_to(before[j, pl.ds(x, 1), :], (8, 128))) * scale
            return carry

        lax.fori_loop(0, cells // BLOCK, body, 0)
        copy = pltpu.make_async_copy(held.at[y], out.at[y], done.at[y])
        copy.start()

    @pl.when(core[0] == 0)
    def _():
        for y in range(2 * half):
            fill(y, (mine, theirs)[y // half], y % half)

    @pl.when(core[0] != 0)
    def _():
        for y in range(2 * half):
            fill(y, (theirs, mine)[y // half], y % half)

    for y in range(2 * half):
        pltpu.make_async_copy(held.at[y], out.at[y], done.at[y]).wait()


def sent(array, axis, by):
    size = lax.axis_size(axis)
    return lax.ppermute(array, axis, [(i, (i + by) % size) for i in range(size)])


def local(field_values, flow_y, flow_x, flow_z):
    core, field_values = lax.optimization_barrier((lax.axis_index("core").reshape(1), field_values))
    height, cells = field_values.shape[:2]
    flows = (flow_y, flow_x, flow_z)
    row = shape(cells, 8, 128)
    inner = shape(height - 2, cells, 8, 128)
    whole = shape(*field_values.shape)
    edge, side = shape(height, cells, 128), shape(height, 8, 128)
    field = (field_values,)
    low, high = call(rows_kernel, (row, row), field_values, in_specs=[IN_HBM], scratch=[pltpu.SemaphoreType.DMA((2,))])
    for _ in range(STEPS):
        parts = len(field)
        slo, shi = sent(high, "south", 1), sent(low, "south", -1)
        first, last, left, right = call(
            functools.partial(faces_kernel, parts, height), (edge, edge, side, side), *field
        )
        downs = (sent(last, DOWN, 1), sent(first, DOWN, -1))
        sides = (sent(right, "east", 1), sent(left, "east", -1))
        (mid,) = call(
            functools.partial(inner_kernel, parts, height), (inner,), *(*field, *downs, *flows), flops=1 << 23
        )
        mid, low, high = call(
            functools.partial(rim_kernel, parts, height),
            (inner, row, row),
            *(*field, *downs, *flows, *sides, slo, shi, mid),
            alias={parts + 9: 0},
        )
        field = (low, mid, high)
    scalar = pl.BlockSpec(memory_space=pltpu.SMEM)
    quarter = shape(height // 2, cells, 128)
    own, other, end = call(
        totals_kernel,
        (quarter, quarter, whole),
        *(core, *field),
        in_specs=[scalar, *[IN_VMEM] * 3],
        out_specs=[IN_VMEM, IN_VMEM, IN_HBM],
        scratch=[pltpu.SemaphoreType.DMA((3,))],
    )
    got = sent(other, "core", 1)
    (total,) = call(add_kernel, (quarter,), own, got)
    chips = lax.axis_size("chip")
    pieces = lax.all_to_all(total.reshape(chips, -1, 128), "chip", 0, 0, tiled=True)
    (pieces,) = call(before_kernel, (shape(*pieces.shape),), pieces)
    below = lax.all_to_all(pieces, "chip", 0, 0, tiled=True).reshape(total.shape)
    mine, partners = call(split_kernel, (quarter, quarter), core, below, own, got, in_specs=[scalar, *[IN_VMEM] * 3])
    theirs = sent(partners, "core", 1)
    (potential,) = call(
        functools.partial(potential_kernel, 1.0 / (8 * chips * 2)),
        (whole,),
        *(core, *field, mine, theirs),
        in_specs=[scalar, *[IN_VMEM] * 5],
        out_specs=[IN_HBM],
        scratch=[pltpu.VMEM(whole.shape, jnp.float32), pltpu.SemaphoreType.DMA((height,))],
    )
    return potential, end


def solution(mesh):
    finer = Mesh(
        mesh.devices.reshape(mesh.shape["south"], mesh.shape["east"], -1, 2), ("south", "east", "chip", "core")
    )
    spec = P("south", "east", DOWN, None)
    return jax.shard_map(local, mesh=finer, in_specs=(spec,) * 4, out_specs=(spec, spec), check_vma=False)
```

```python
import functools

import jax
import jax.numpy as jnp
from jax import lax
from jax.experimental import pallas as pl
from jax.experimental.pallas import tpu as pltpu
from jax.sharding import Mesh
from jax.sharding import PartitionSpec as P

STEPS = 4
RATE = 0.05
BLOCK = 8
GROUP = 3
VMEM = 5 << 20


DOWN = ("chip", "core")
IN_VMEM = pl.BlockSpec(memory_space=pltpu.VMEM)
IN_HBM = pl.BlockSpec(memory_space=pltpu.HBM)


def shape(*dims):
    return jax.ShapeDtypeStruct(dims, jnp.float32)


def call(kernel, outs, *args, flops=1 << 21, in_specs=None, out_specs=None, scratch=(), alias=None, vmem=VMEM):
    return pl.pallas_call(
        kernel,
        out_shape=outs,
        in_specs=in_specs or [IN_VMEM] * len(args),
        out_specs=out_specs or [IN_VMEM] * len(outs),
        scratch_shapes=scratch,
        input_output_aliases=alias or {},
        compiler_params=pltpu.CompilerParams(vmem_limit_bytes=vmem),
        cost_estimate=pl.CostEstimate(flops=flops, bytes_accessed=0, transcendentals=0),
    )(*args)


def advance(here, up, down, left, right, ahead, behind, fy, fx, fz):
    around = ((up + down) + (left + right)) + (ahead + behind)
    carried = (fy * (up - down) + fx * (right - left)) + fz * (ahead - behind)
    return ((1.0 - 6.0 * RATE) * here + RATE * around) - carried


def turned(here):
    return pltpu.roll(here, 7, 0), pltpu.roll(here, 1, 0)


def along_z(here, zlo, zhi, y, x):
    sublane = lax.broadcasted_iota(jnp.int32, (8, 128), 0)
    ahead, behind = turned(here)
    head = jnp.broadcast_to(zhi[y, pl.ds(x, 1), :], (8, 128))
    tail = jnp.broadcast_to(zlo[y, pl.ds(x, 1), :], (8, 128))
    return jnp.where(sublane == 7, head, ahead), jnp.where(sublane == 0, tail, behind)


def march(cells, column_at, cell, left):
    def run(start, first, last, left, mid):
        for k in range(first, last):
            right = column_at(start + k + 1)
            cell(start + k, left, mid, right)
            left, mid = mid, right
        return left, mid

    def body(i, carry):
        return run(pl.multiple_of(i * BLOCK, BLOCK), 0, BLOCK, *carry)

    if left is None:
        carry = run(0, 1, BLOCK, column_at(0), column_at(1))
    else:
        carry = run(0, 0, BLOCK, left, column_at(0))
    carry = lax.fori_loop(1, cells // BLOCK - 1, body, carry)
    return run(cells - BLOCK, 0, BLOCK - 1, *carry)


def reader(ref, *at):
    return lambda x: ref[(*at, x)]


def planes_of(refs, height):
    if len(refs) == 1:
        return [refs[0].at[y] for y in range(height)]
    low, inner, high = refs
    return [low, *(inner.at[y] for y in range(height - 2)), high]


def pack(plane, at):
    cells = plane.shape[0]
    return plane.reshape(cells * 8, 128)[pl.ds(at, cells, 8), :]


def inner_kernel(parts, height, *refs):
    field, (fy, fx, fz), out = refs[:parts], refs[parts : parts + 3], refs[parts + 3]
    cells = fy.shape[1]
    rows = [reader(plane) for plane in planes_of(field, height)]
    for start in range(1, height - 1, GROUP):
        ys = list(range(start, min(start + GROUP, height - 1)))

        def cell(x, left, mid, right, ys=ys):
            column = [rows[ys[0] - 1](x), *mid, rows[ys[-1] + 1](x)]
            for g, y in enumerate(ys):
                out[y - 1, x] = advance(
                    mid[g], column[g + 2], column[g], left[g], right[g], *turned(mid[g]), fy[y, x], fx[y, x], fz[y, x]
                )

        march(cells, lambda x, ys=ys: [rows[y](x) for y in ys], cell, None)


def mend_kernel(parts, height, *refs):
    field, (fy, fx, fz) = refs[:parts], refs[parts : parts + 3]
    (zlo, zhi), (first, last) = refs[parts + 3 : parts + 5], refs[parts + 5 : parts + 7]
    to_first, to_last = refs[parts + 7 : parts + 9]
    sides, out = refs[parts + 9 : parts + 11], refs[parts + 12]
    cells = fy.shape[1]
    rows = [reader(plane) for plane in planes_of(field, height)]
    for y in range(1, height - 1):
        flat = out.at[y - 1].reshape(cells * 8, 128)
        flat[pl.ds(0, cells, 8), :] += to_first[y] * (zlo[y] - last[y])
        flat[pl.ds(7, cells, 8), :] += to_last[y] * (zhi[y] - first[y])
        for x, left, right in (
            (0, sides[0][y], rows[y](1)),
            (cells - 1, rows[y](cells - 2), sides[1][y]),
        ):
            here = rows[y](x)
            out[y - 1, x] = advance(
                *(here, rows[y + 1](x), rows[y - 1](x), left, right),
                *along_z(here, zlo, zhi, y, x),
                *(fy[y, x], fx[y, x], fz[y, x]),
            )


def rim_kernel(parts, height, top, *refs):
    field, (fy, fx, fz) = refs[:parts], refs[parts : parts + 3]
    (zlo, zhi), sides = refs[parts + 3 : parts + 5], refs[parts + 5 : parts + 7]
    beyond, out = refs[parts + 7 :]
    cells = fy.shape[1]
    rows = [reader(plane) for plane in planes_of(field, height)]
    y = height - 1 if top else 0
    here = rows[y]
    above, below = (reader(beyond), rows[y - 1]) if top else (rows[1], reader(beyond))

    def cell(x, left, mid, right):
        out[x] = advance(
            mid, above(x), below(x), left, right, *along_z(mid, zlo, zhi, y, x), fy[y, x], fx[y, x], fz[y, x]
        )

    carry = march(cells, here, cell, sides[0][y])
    cell(cells - 1, *carry, sides[1][y])


def near_kernel(fz, to_first, to_last):
    for y in range(fz.shape[0]):
        to_first[y] = RATE + pack(fz.at[y], 0)
        to_last[y] = RATE - pack(fz.at[y], 7)


def rows_kernel(field, low, high, done):
    copies = [
        pltpu.make_async_copy(field.at[0], low, done.at[0]),
        pltpu.make_async_copy(field.at[field.shape[0] - 1], high, done.at[1]),
    ]
    for copy in copies:
        copy.start()
    for copy in copies:
        copy.wait()


def faces_kernel(parts, height, *refs):
    field, (first, last, left, right) = refs[:parts], refs[parts:]
    for y, plane in enumerate(planes_of(field, height)):
        first[y] = pack(plane, 0)
        last[y] = pack(plane, 7)
        left[y] = plane[0]
        right[y] = plane[plane.shape[0] - 1]


def running_sums(scale, plane, put):
    sublane = lax.broadcasted_iota(jnp.int32, (8, 128), 0)

    def body(i, carry):
        start = pl.multiple_of(i * BLOCK, BLOCK)
        for k in range(BLOCK):
            value = plane[start + k] * scale
            for reach in (1, 2, 4):
                value = value + jnp.where(sublane >= reach, pltpu.roll(value, reach, 0), 0.0)
            put(start + k, value)
        return carry

    lax.fori_loop(0, plane.shape[0] // BLOCK, body, 0)


def inner_sums_kernel(scale, inner, held, end, done):
    count = inner.shape[0]
    copy = pltpu.make_async_copy(inner, end.at[pl.ds(1, count)], done.at[0])
    copy.start()
    for y in range(count):

        def put(x, value, y=y):
            held[y, x] = value

        running_sums(scale, inner.at[y], put)
    copy.wait()


def rim_sums_kernel(scale, core, low, high, inner_held, end_in, own, other, held, end, done):
    half = own.shape[0]
    copies = [
        pltpu.make_async_copy(low, end.at[0], done.at[0]),
        pltpu.make_async_copy(high, end.at[2 * half - 1], done.at[1]),
    ]
    for copy in copies:
        copy.start()
    for k, plane in enumerate((low, high)):

        def put(x, value, k=k):
            held[k, x] = value

        running_sums(scale, plane, put)
    planes = planes_of((held.at[0], inner_held, held.at[1]), 2 * half)

    @pl.when(core[0] == 0)
    def _():
        for y in range(half):
            own[y] = pack(planes[y], 7)
            other[y] = pack(planes[half + y], 7)

    @pl.when(core[0] != 0)
    def _():
        for y in range(half):
            own[y] = pack(planes[half + y], 7)
            other[y] = pack(planes[y], 7)

    for copy in copies:
        copy.wait()


def add_kernel(a, b, out):
    out[...] = a[...] + b[...]


def before_kernel(pieces, out):
    so_far = jnp.zeros(pieces.shape[1:], jnp.float32)
    for k in range(pieces.shape[0]):
        out[k] = so_far
        so_far = so_far + pieces[k]


def split_kernel(core, chips, own, got, mine, partners):
    @pl.when(core[0] == 0)
    def _():
        mine[...] = chips[...]
        partners[...] = chips[...] + own[...]

    @pl.when(core[0] != 0)
    def _():
        mine[...] = chips[...] + got[...]
        partners[...] = chips[...]


def potential_kernel(core, inner_held, rim_held, mine, theirs, out, done_rows, done):
    half, cells = mine.shape[:2]
    planes = planes_of((rim_held.at[0], inner_held, rim_held.at[1]), 2 * half)

    def fill(y, before, j):
        def body(i, carry):
            start = pl.multiple_of(i * BLOCK, BLOCK)
            for k in range(BLOCK):
                x = start + k
                done_rows[y, x] = planes[y][x] + jnp.broadcast_to(before[j, pl.ds(x, 1), :], (8, 128))
            return carry

        lax.fori_loop(0, cells // BLOCK, body, 0)
        pltpu.make_async_copy(done_rows.at[y], out.at[y], done.at[y]).start()

    @pl.when(core[0] == 0)
    def _():
        for y in range(2 * half):
            fill(y, (mine, theirs)[y // half], y % half)

    @pl.when(core[0] != 0)
    def _():
        for y in range(2 * half):
            fill(y, (theirs, mine)[y // half], y % half)

    for y in range(2 * half):
        pltpu.make_async_copy(done_rows.at[y], out.at[y], done.at[y]).wait()


def sent(array, axis, by):
    size = lax.axis_size(axis)
    return lax.ppermute(array, axis, [(i, (i + by) % size) for i in range(size)])


def local(field_values, flow_y, flow_x, flow_z):
    core, field_values = lax.optimization_barrier((lax.axis_index("core").reshape(1), field_values))
    height, cells = field_values.shape[:2]
    flows = (flow_y, flow_x, flow_z)
    row, pair = shape(cells, 8, 128), shape(2, cells, 8, 128)
    inner = shape(height - 2, cells, 8, 128)
    whole = shape(*field_values.shape)
    edge, side = shape(height, cells, 128), shape(height, 8, 128)
    scalar = pl.BlockSpec(memory_space=pltpu.SMEM)

    def send_faces(field):
        first, last, left, right = call(
            functools.partial(faces_kernel, len(field), height), (edge, edge, side, side), *field
        )
        downs = sent(last, DOWN, 1), sent(first, DOWN, -1)
        sides = sent(right, "east", 1), sent(left, "east", -1)
        return (first, last), downs, sides

    def send_rim(low, high):
        return sent(high, "south", 1), sent(low, "south", -1)

    low, high = call(
        rows_kernel, (row, row), field_values, in_specs=[IN_HBM], scratch=[pltpu.SemaphoreType.DMA((2,))], vmem=52 << 20
    )
    slo, shi = send_rim(low, high)
    field = (field_values,)
    faces, downs, sides = send_faces(field)
    near = call(near_kernel, (edge, edge), flow_z)
    for step in range(1, STEPS + 1):
        parts = len(field)
        (mid,) = call(functools.partial(inner_kernel, parts, height), (inner,), *(*field, *flows), flops=1 << 23)
        (mid,) = call(
            functools.partial(mend_kernel, parts, height),
            (inner,),
            *(*field, *flows, *downs, *faces, *near, *sides, mid),
            alias={parts + 11: 0},
        )
        low, high = (
            call(
                functools.partial(rim_kernel, parts, height, top), (row,), *(*field, *flows, *downs, *sides, beyond)
            )[0]
            for top, beyond in ((False, slo), (True, shi))
        )
        field = (low, mid, high)
        if step < STEPS:
            slo, shi = send_rim(low, high)
            faces, downs, sides = send_faces(field)
    chips = lax.axis_size("chip")
    scale = 1.0 / (8 * chips * 2)
    inner_held, end = call(
        functools.partial(inner_sums_kernel, scale),
        (inner, whole),
        mid,
        out_specs=[IN_VMEM, IN_HBM],
        scratch=[pltpu.SemaphoreType.DMA((1,))],
    )
    quarter = shape(height // 2, cells, 128)
    own, other, rim_held, end = call(
        functools.partial(rim_sums_kernel, scale),
        (quarter, quarter, pair, whole),
        *(core, low, high, inner_held, end),
        in_specs=[scalar, *[IN_VMEM] * 3, IN_HBM],
        out_specs=[*[IN_VMEM] * 3, IN_HBM],
        scratch=[pltpu.SemaphoreType.DMA((2,))],
        alias={4: 3},
    )
    got = sent(other, "core", 1)
    (total,) = call(add_kernel, (quarter,), own, got)
    pieces = lax.all_to_all(total.reshape(chips, -1, 128), "chip", 0, 0, tiled=True)
    (pieces,) = call(before_kernel, (shape(*pieces.shape),), pieces)
    below = lax.all_to_all(pieces, "chip", 0, 0, tiled=True).reshape(total.shape)
    mine, partners = call(split_kernel, (quarter, quarter), core, below, own, got, in_specs=[scalar, *[IN_VMEM] * 3])
    theirs = sent(partners, "core", 1)
    (potential,) = call(
        potential_kernel,
        (whole,),
        *(core, inner_held, rim_held, mine, theirs),
        in_specs=[scalar, *[IN_VMEM] * 4],
        out_specs=[IN_HBM],
        scratch=[pltpu.VMEM(whole.shape, jnp.float32), pltpu.SemaphoreType.DMA((height,))],
    )
    return potential, end


def solution(mesh):
    finer = Mesh(
        mesh.devices.reshape(mesh.shape["south"], mesh.shape["east"], -1, 2), ("south", "east", "chip", "core")
    )
    spec = P("south", "east", DOWN, None)
    return jax.shard_map(local, mesh=finer, in_specs=(spec,) * 4, out_specs=(spec, spec), check_vma=False)
```

```python
import functools

import jax
import jax.numpy as jnp
from jax import lax
from jax.experimental import pallas as pl
from jax.experimental.pallas import tpu as pltpu
from jax.sharding import Mesh
from jax.sharding import PartitionSpec as P

STEPS = 4
RATE = 0.05
BLOCK = 8
GROUP = 3
VMEM = 5 << 20


DOWN = ("chip", "core")
IN_VMEM = pl.BlockSpec(memory_space=pltpu.VMEM)
IN_HBM = pl.BlockSpec(memory_space=pltpu.HBM)


def shape(*dims):
    return jax.ShapeDtypeStruct(dims, jnp.float32)


def call(kernel, outs, *args, flops=1 << 21, in_specs=None, out_specs=None, scratch=(), alias=None, vmem=VMEM):
    return pl.pallas_call(
        kernel,
        out_shape=outs,
        in_specs=in_specs or [IN_VMEM] * len(args),
        out_specs=out_specs or [IN_VMEM] * len(outs),
        scratch_shapes=scratch,
        input_output_aliases=alias or {},
        compiler_params=pltpu.CompilerParams(vmem_limit_bytes=vmem),
        cost_estimate=pl.CostEstimate(flops=flops, bytes_accessed=0, transcendentals=0),
    )(*args)


def advance(here, up, down, left, right, ahead, behind, fy, fx, fz):
    around = ((up + down) + (left + right)) + (ahead + behind)
    carried = (fy * (up - down) + fx * (right - left)) + fz * (ahead - behind)
    return ((1.0 - 6.0 * RATE) * here + RATE * around) - carried


def turned(here):
    return pltpu.roll(here, 7, 0), pltpu.roll(here, 1, 0)


def along_z(here, zlo, zhi, y, x):
    sublane = lax.broadcasted_iota(jnp.int32, (8, 128), 0)
    ahead, behind = turned(here)
    head = jnp.broadcast_to(zhi[y, pl.ds(x, 1), :], (8, 128))
    tail = jnp.broadcast_to(zlo[y, pl.ds(x, 1), :], (8, 128))
    return jnp.where(sublane == 7, head, ahead), jnp.where(sublane == 0, tail, behind)


def march(cells, column_at, cell, left):
    def run(start, first, last, left, mid):
        for k in range(first, last):
            right = column_at(start + k + 1)
            cell(start + k, left, mid, right)
            left, mid = mid, right
        return left, mid

    def body(i, carry):
        return run(pl.multiple_of(i * BLOCK, BLOCK), 0, BLOCK, *carry)

    if left is None:
        carry = run(0, 1, BLOCK, column_at(0), column_at(1))
    else:
        carry = run(0, 0, BLOCK, left, column_at(0))
    carry = lax.fori_loop(1, cells // BLOCK - 1, body, carry)
    return run(cells - BLOCK, 0, BLOCK - 1, *carry)


def reader(ref, *at):
    return lambda x: ref[(*at, x)]


def planes_of(refs, height):
    if len(refs) == 1:
        return [refs[0].at[y] for y in range(height)]
    low, inner, high = refs
    return [low, *(inner.at[y] for y in range(height - 2)), high]


def pack(plane, at):
    cells = plane.shape[0]
    return plane.reshape(cells * 8, 128)[pl.ds(at, cells, 8), :]


def inner_kernel(parts, height, *refs):
    field, (fy, fx, fz), out = refs[:parts], refs[parts : parts + 3], refs[parts + 3]
    cells = fy.shape[1]
    rows = [reader(plane) for plane in planes_of(field, height)]
    for start in range(1, height - 1, GROUP):
        ys = list(range(start, min(start + GROUP, height - 1)))

        def cell(x, left, mid, right, ys=ys):
            column = [rows[ys[0] - 1](x), *mid, rows[ys[-1] + 1](x)]
            for g, y in enumerate(ys):
                out[y - 1, x] = advance(
                    mid[g], column[g + 2], column[g], left[g], right[g], *turned(mid[g]), fy[y, x], fx[y, x], fz[y, x]
                )

        march(cells, lambda x, ys=ys: [rows[y](x) for y in ys], cell, None)


def mend_kernel(parts, height, *refs):
    field, (fy, fx, fz) = refs[:parts], refs[parts : parts + 3]
    (zlo, zhi), (first, last) = refs[parts + 3 : parts + 5], refs[parts + 5 : parts + 7]
    to_first, to_last = refs[parts + 7 : parts + 9]
    sides, out = refs[parts + 9 : parts + 11], refs[parts + 12]
    cells = fy.shape[1]
    rows = [reader(plane) for plane in planes_of(field, height)]
    for y in range(1, height - 1):
        flat = out.at[y - 1].reshape(cells * 8, 128)
        flat[pl.ds(0, cells, 8), :] += to_first[y] * (zlo[y] - last[y])
        flat[pl.ds(7, cells, 8), :] += to_last[y] * (zhi[y] - first[y])
        for x, left, right in (
            (0, sides[0][y], rows[y](1)),
            (cells - 1, rows[y](cells - 2), sides[1][y]),
        ):
            here = rows[y](x)
            out[y - 1, x] = advance(
                *(here, rows[y + 1](x), rows[y - 1](x), left, right),
                *along_z(here, zlo, zhi, y, x),
                *(fy[y, x], fx[y, x], fz[y, x]),
            )


def rim_kernel(parts, height, top, *refs):
    field, (fy, fx, fz) = refs[:parts], refs[parts : parts + 3]
    (zlo, zhi), sides = refs[parts + 3 : parts + 5], refs[parts + 5 : parts + 7]
    beyond, out = refs[parts + 7 :]
    cells = fy.shape[1]
    rows = [reader(plane) for plane in planes_of(field, height)]
    y = height - 1 if top else 0
    here = rows[y]
    above, below = (reader(beyond), rows[y - 1]) if top else (rows[1], reader(beyond))

    def cell(x, left, mid, right):
        out[x] = advance(
            mid, above(x), below(x), left, right, *along_z(mid, zlo, zhi, y, x), fy[y, x], fx[y, x], fz[y, x]
        )

    carry = march(cells, here, cell, sides[0][y])
    cell(cells - 1, *carry, sides[1][y])


def near_kernel(fz, to_first, to_last):
    for y in range(fz.shape[0]):
        to_first[y] = RATE + pack(fz.at[y], 0)
        to_last[y] = RATE - pack(fz.at[y], 7)


def rows_kernel(field, low, high, done):
    copies = [
        pltpu.make_async_copy(field.at[0], low, done.at[0]),
        pltpu.make_async_copy(field.at[field.shape[0] - 1], high, done.at[1]),
    ]
    for copy in copies:
        copy.start()
    for copy in copies:
        copy.wait()


def faces_kernel(parts, height, *refs):
    field, (first, last, left, right) = refs[:parts], refs[parts:]
    for y, plane in enumerate(planes_of(field, height)):
        first[y] = pack(plane, 0)
        last[y] = pack(plane, 7)
        left[y] = plane[0]
        right[y] = plane[plane.shape[0] - 1]


def running_sums(scale, plane, put):
    sublane = lax.broadcasted_iota(jnp.int32, (8, 128), 0)

    def body(i, carry):
        start = pl.multiple_of(i * BLOCK, BLOCK)
        for k in range(BLOCK):
            value = plane[start + k] * scale
            for reach in (1, 2, 4):
                value = value + jnp.where(sublane >= reach, pltpu.roll(value, reach, 0), 0.0)
            put(start + k, value)
        return carry

    lax.fori_loop(0, plane.shape[0] // BLOCK, body, 0)


def inner_sums_kernel(scale, inner, held, end, done):
    count = inner.shape[0]
    copy = pltpu.make_async_copy(inner, end.at[pl.ds(1, count)], done.at[0])
    copy.start()
    for y in range(count):

        def put(x, value, y=y):
            held[y, x] = value

        running_sums(scale, inner.at[y], put)
    copy.wait()


def rim_sums_kernel(scale, core, low, high, inner_held, own, other, held):
    half = own.shape[0]
    for k, plane in enumerate((low, high)):

        def put(x, value, k=k):
            held[k, x] = value

        running_sums(scale, plane, put)
    planes = planes_of((held.at[0], inner_held, held.at[1]), 2 * half)

    @pl.when(core[0] == 0)
    def _():
        for y in range(half):
            own[y] = pack(planes[y], 7)
            other[y] = pack(planes[half + y], 7)

    @pl.when(core[0] != 0)
    def _():
        for y in range(half):
            own[y] = pack(planes[half + y], 7)
            other[y] = pack(planes[y], 7)


def add_kernel(a, b, out):
    out[...] = a[...] + b[...]


def before_kernel(pieces, out):
    so_far = jnp.zeros(pieces.shape[1:], jnp.float32)
    for k in range(pieces.shape[0]):
        out[k] = so_far
        so_far = so_far + pieces[k]


def split_kernel(core, chips, own, got, mine, partners):
    @pl.when(core[0] == 0)
    def _():
        mine[...] = chips[...]
        partners[...] = chips[...] + own[...]

    @pl.when(core[0] != 0)
    def _():
        mine[...] = chips[...] + got[...]
        partners[...] = chips[...]


def half_potential(side, inner_held, rim_held, before, out, filled, done):
    half, cells = before.shape[:2]
    planes = planes_of((rim_held.at[0], inner_held, rim_held.at[1]), 2 * half)

    def fill(which):
        for j in range(half):
            y = which * half + j

            def body(i, carry, y=y, j=j):
                start = pl.multiple_of(i * BLOCK, BLOCK)
                for k in range(BLOCK):
                    x = start + k
                    filled[j, x] = planes[y][x] + jnp.broadcast_to(before[j, pl.ds(x, 1), :], (8, 128))
                return carry

            lax.fori_loop(0, cells // BLOCK, body, 0)
            pltpu.make_async_copy(filled.at[j], out.at[y], done.at[j]).start()
        for j in range(half):
            pltpu.make_async_copy(filled.at[j], out.at[which * half + j], done.at[j]).wait()

    @pl.when(side == 0)
    def _():
        fill(0)

    @pl.when(side != 0)
    def _():
        fill(1)


def own_half_kernel(core, low, high, inner_held, rim_held, before, end_in, out, end, filled, done, done_rims):
    copies = [
        pltpu.make_async_copy(low, end.at[0], done_rims.at[0]),
        pltpu.make_async_copy(high, end.at[end.shape[0] - 1], done_rims.at[1]),
    ]
    for copy in copies:
        copy.start()
    half_potential(core[0], inner_held, rim_held, before, out, filled, done)
    for copy in copies:
        copy.wait()


def other_half_kernel(core, inner_held, rim_held, before, out_in, out, filled, done):
    half_potential(1 - core[0], inner_held, rim_held, before, out, filled, done)


def sent(array, axis, by):
    size = lax.axis_size(axis)
    return lax.ppermute(array, axis, [(i, (i + by) % size) for i in range(size)])


def local(field_values, flow_y, flow_x, flow_z):
    core, field_values = lax.optimization_barrier((lax.axis_index("core").reshape(1), field_values))
    height, cells = field_values.shape[:2]
    flows = (flow_y, flow_x, flow_z)
    row, pair = shape(cells, 8, 128), shape(2, cells, 8, 128)
    inner = shape(height - 2, cells, 8, 128)
    whole = shape(*field_values.shape)
    edge, side = shape(height, cells, 128), shape(height, 8, 128)
    scalar = pl.BlockSpec(memory_space=pltpu.SMEM)

    def send_faces(field):
        first, last, left, right = call(
            functools.partial(faces_kernel, len(field), height), (edge, edge, side, side), *field
        )
        downs = sent(last, DOWN, 1), sent(first, DOWN, -1)
        sides = sent(right, "east", 1), sent(left, "east", -1)
        return (first, last), downs, sides

    def send_rim(low, high):
        return sent(high, "south", 1), sent(low, "south", -1)

    low, high = call(
        rows_kernel, (row, row), field_values, in_specs=[IN_HBM], scratch=[pltpu.SemaphoreType.DMA((2,))], vmem=48 << 20
    )
    slo, shi = send_rim(low, high)
    field = (field_values,)
    faces, downs, sides = send_faces(field)
    near = call(near_kernel, (edge, edge), flow_z)
    for step in range(1, STEPS + 1):
        parts = len(field)
        (mid,) = call(functools.partial(inner_kernel, parts, height), (inner,), *(*field, *flows), flops=1 << 23)
        (mid,) = call(
            functools.partial(mend_kernel, parts, height),
            (inner,),
            *(*field, *flows, *downs, *faces, *near, *sides, mid),
            alias={parts + 11: 0},
        )
        low, high = (
            call(
                functools.partial(rim_kernel, parts, height, top), (row,), *(*field, *flows, *downs, *sides, beyond)
            )[0]
            for top, beyond in ((False, slo), (True, shi))
        )
        field = (low, mid, high)
        if step < STEPS:
            slo, shi = send_rim(low, high)
            faces, downs, sides = send_faces(field)
    chips = lax.axis_size("chip")
    scale = 1.0 / (8 * chips * 2)
    inner_held, end = call(
        functools.partial(inner_sums_kernel, scale),
        (inner, whole),
        mid,
        out_specs=[IN_VMEM, IN_HBM],
        scratch=[pltpu.SemaphoreType.DMA((1,))],
    )
    quarter = shape(height // 2, cells, 128)
    own, other, rim_held = call(
        functools.partial(rim_sums_kernel, scale),
        (quarter, quarter, pair),
        *(core, low, high, inner_held),
        in_specs=[scalar, *[IN_VMEM] * 3],
    )
    got = sent(other, "core", 1)
    (total,) = call(add_kernel, (quarter,), own, got)
    pieces = lax.all_to_all(total.reshape(chips, -1, 128), "chip", 0, 0, tiled=True)
    (pieces,) = call(before_kernel, (shape(*pieces.shape),), pieces)
    below = lax.all_to_all(pieces, "chip", 0, 0, tiled=True).reshape(total.shape)
    mine, partners = call(split_kernel, (quarter, quarter), core, below, own, got, in_specs=[scalar, *[IN_VMEM] * 3])
    theirs = sent(partners, "core", 1)
    rows_out = [pltpu.VMEM((height // 2, cells, 8, 128), jnp.float32), pltpu.SemaphoreType.DMA((height // 2,))]
    potential, end = call(
        own_half_kernel,
        (whole, whole),
        *(core, low, high, inner_held, rim_held, mine, end),
        in_specs=[scalar, *[IN_VMEM] * 5, IN_HBM],
        out_specs=[IN_HBM, IN_HBM],
        scratch=[*rows_out, pltpu.SemaphoreType.DMA((2,))],
        alias={6: 1},
    )
    (potential,) = call(
        other_half_kernel,
        (whole,),
        *(core, inner_held, rim_held, theirs, potential),
        in_specs=[scalar, *[IN_VMEM] * 3, IN_HBM],
        out_specs=[IN_HBM],
        scratch=rows_out,
        alias={4: 0},
    )
    return potential, end


def solution(mesh):
    finer = Mesh(
        mesh.devices.reshape(mesh.shape["south"], mesh.shape["east"], -1, 2), ("south", "east", "chip", "core")
    )
    spec = P("south", "east", DOWN, None)
    return jax.shard_map(local, mesh=finer, in_specs=(spec,) * 4, out_specs=(spec, spec), check_vma=False)
```

```python
import functools

import jax
import jax.numpy as jnp
from jax import lax
from jax.experimental import pallas as pl
from jax.experimental.pallas import tpu as pltpu
from jax.sharding import Mesh
from jax.sharding import PartitionSpec as P

STEPS = 4
RATE = 0.05
BLOCK = 8
GROUP = 4
VMEM = 5 << 20


DOWN = ("chip", "core")
IN_VMEM = pl.BlockSpec(memory_space=pltpu.VMEM)
IN_HBM = pl.BlockSpec(memory_space=pltpu.HBM)


def shape(*dims):
    return jax.ShapeDtypeStruct(dims, jnp.float32)


def call(kernel, outs, *args, flops=1 << 21, in_specs=None, out_specs=None, scratch=(), alias=None, vmem=VMEM):
    return pl.pallas_call(
        kernel,
        out_shape=outs,
        in_specs=in_specs or [IN_VMEM] * len(args),
        out_specs=out_specs or [IN_VMEM] * len(outs),
        scratch_shapes=scratch,
        input_output_aliases=alias or {},
        compiler_params=pltpu.CompilerParams(vmem_limit_bytes=vmem),
        cost_estimate=pl.CostEstimate(flops=flops, bytes_accessed=0, transcendentals=0),
    )(*args)


def advance(here, up, down, left, right, ahead, behind, fy, fx, fz):
    around = ((up + down) + (left + right)) + (ahead + behind)
    carried = (fy * (up - down) + fx * (right - left)) + fz * (ahead - behind)
    return ((1.0 - 6.0 * RATE) * here + RATE * around) - carried


def turned(here):
    return pltpu.roll(here, 7, 0), pltpu.roll(here, 1, 0)


def along_z(here, zlo, zhi, y, x):
    sublane = lax.broadcasted_iota(jnp.int32, (8, 128), 0)
    ahead, behind = turned(here)
    head = jnp.broadcast_to(zhi[y, pl.ds(x, 1), :], (8, 128))
    tail = jnp.broadcast_to(zlo[y, pl.ds(x, 1), :], (8, 128))
    return jnp.where(sublane == 7, head, ahead), jnp.where(sublane == 0, tail, behind)


def march(cells, column_at, cell):
    def run(start, first, last, left, mid):
        for k in range(first, last):
            right = column_at(start + k + 1)
            cell(start + k, left, mid, right)
            left, mid = mid, right
        return left, mid

    def body(i, carry):
        return run(pl.multiple_of(i * BLOCK, BLOCK), 0, BLOCK, *carry)

    carry = run(0, 1, BLOCK, column_at(0), column_at(1))
    carry = lax.fori_loop(1, cells // BLOCK - 1, body, carry)
    run(cells - BLOCK, 0, BLOCK - 1, *carry)


def reader(ref, *at):
    return lambda x: ref[(*at, x)]


def planes_of(refs, height):
    if len(refs) == 1:
        return [refs[0].at[y] for y in range(height)]
    low, inner, high = refs
    return [low, *(inner.at[y] for y in range(height - 2)), high]


def pack(plane, at):
    cells = plane.shape[0]
    return plane.reshape(cells * 8, 128)[pl.ds(at, cells, 8), :]


def inner_kernel(parts, height, *refs):
    field, (fy, fx, fz), (out, low, high) = refs[:parts], refs[parts : parts + 3], refs[parts + 3 :]
    cells = fy.shape[1]
    planes = [low, *(out.at[y] for y in range(height - 2)), high]
    nothing = lambda x: jnp.zeros((8, 128), jnp.float32)
    rows = [nothing, *(reader(plane) for plane in planes_of(field, height)), nothing]
    for start in range(0, height, GROUP):
        ys = list(range(start, min(start + GROUP, height)))

        def cell(x, left, mid, right, ys=ys):
            column = [rows[ys[0]](x), *mid, rows[ys[-1] + 2](x)]
            for g, y in enumerate(ys):
                planes[y][x] = advance(
                    mid[g], column[g + 2], column[g], left[g], right[g], *turned(mid[g]), fy[y, x], fx[y, x], fz[y, x]
                )

        march(cells, lambda x, ys=ys: [rows[y + 1](x) for y in ys], cell)


def mend_kernel(parts, height, *refs):
    field, (fy, fx, fz) = refs[:parts], refs[parts : parts + 3]
    (zlo, zhi), (first, last) = refs[parts + 3 : parts + 5], refs[parts + 5 : parts + 7]
    to_first, to_last = refs[parts + 7 : parts + 9]
    sides, out = refs[parts + 9 : parts + 11], refs[parts + 12]
    cells = fy.shape[1]
    rows = [reader(plane) for plane in planes_of(field, height)]
    for y in range(1, height - 1):
        flat = out.at[y - 1].reshape(cells * 8, 128)
        flat[pl.ds(0, cells, 8), :] += to_first[y] * (zlo[y] - last[y])
        flat[pl.ds(7, cells, 8), :] += to_last[y] * (zhi[y] - first[y])
        for x, left, right in (
            (0, sides[0][y], rows[y](1)),
            (cells - 1, rows[y](cells - 2), sides[1][y]),
        ):
            here = rows[y](x)
            out[y - 1, x] = advance(
                *(here, rows[y + 1](x), rows[y - 1](x), left, right),
                *along_z(here, zlo, zhi, y, x),
                *(fy[y, x], fx[y, x], fz[y, x]),
            )


def rim_kernel(parts, height, top, *refs):
    field, (fy, fx, fz) = refs[:parts], refs[parts : parts + 3]
    (zlo, zhi), (first, last) = refs[parts + 3 : parts + 5], refs[parts + 5 : parts + 7]
    to_first, to_last = refs[parts + 7 : parts + 9]
    sides, beyond, out = refs[parts + 9 : parts + 11], refs[parts + 11], refs[parts + 13]
    cells = fy.shape[1]
    rows = [reader(plane) for plane in planes_of(field, height)]
    y = height - 1 if top else 0

    def body(i, carry):
        start = pl.multiple_of(i * BLOCK, BLOCK)
        for k in range(BLOCK):
            x = start + k
            rate = RATE - fy[y, x] if top else RATE + fy[y, x]
            out[x] += rate * beyond[x]
        return carry

    lax.fori_loop(0, cells // BLOCK, body, 0)
    flat = out.reshape(cells * 8, 128)
    flat[pl.ds(0, cells, 8), :] += to_first[y] * (zlo[y] - last[y])
    flat[pl.ds(7, cells, 8), :] += to_last[y] * (zhi[y] - first[y])
    above, below = (reader(beyond), rows[y - 1]) if top else (rows[1], reader(beyond))
    for x, left, right in (
        (0, sides[0][y], rows[y](1)),
        (cells - 1, rows[y](cells - 2), sides[1][y]),
    ):
        here = rows[y](x)
        out[x] = advance(
            *(here, above(x), below(x), left, right),
            *along_z(here, zlo, zhi, y, x),
            *(fy[y, x], fx[y, x], fz[y, x]),
        )


def near_kernel(fz, to_first, to_last):
    for y in range(fz.shape[0]):
        to_first[y] = RATE + pack(fz.at[y], 0)
        to_last[y] = RATE - pack(fz.at[y], 7)


def rows_kernel(field, low, high, done):
    copies = [
        pltpu.make_async_copy(field.at[0], low, done.at[0]),
        pltpu.make_async_copy(field.at[field.shape[0] - 1], high, done.at[1]),
    ]
    for copy in copies:
        copy.start()
    for copy in copies:
        copy.wait()


def faces_kernel(parts, height, *refs):
    field, (first, last, left, right) = refs[:parts], refs[parts:]
    for y, plane in enumerate(planes_of(field, height)):
        first[y] = pack(plane, 0)
        last[y] = pack(plane, 7)
        left[y] = plane[0]
        right[y] = plane[plane.shape[0] - 1]


def running_sums(scale, plane, put):
    sublane = lax.broadcasted_iota(jnp.int32, (8, 128), 0)

    def body(i, carry):
        start = pl.multiple_of(i * BLOCK, BLOCK)
        for k in range(BLOCK):
            value = plane[start + k] * scale
            for reach in (1, 2, 4):
                value = value + jnp.where(sublane >= reach, pltpu.roll(value, reach, 0), 0.0)
            put(start + k, value)
        return carry

    lax.fori_loop(0, plane.shape[0] // BLOCK, body, 0)


def inner_sums_kernel(scale, inner, held, end, done):
    count = inner.shape[0]
    copy = pltpu.make_async_copy(inner, end.at[pl.ds(1, count)], done.at[0])
    copy.start()
    for y in range(count):

        def put(x, value, y=y):
            held[y, x] = value

        running_sums(scale, inner.at[y], put)
    copy.wait()


def rim_sums_kernel(scale, core, low, high, inner_held, own, other, held):
    half = own.shape[0]
    for k, plane in enumerate((low, high)):

        def put(x, value, k=k):
            held[k, x] = value

        running_sums(scale, plane, put)
    planes = planes_of((held.at[0], inner_held, held.at[1]), 2 * half)

    @pl.when(core[0] == 0)
    def _():
        for y in range(half):
            own[y] = pack(planes[y], 7)
            other[y] = pack(planes[half + y], 7)

    @pl.when(core[0] != 0)
    def _():
        for y in range(half):
            own[y] = pack(planes[half + y], 7)
            other[y] = pack(planes[y], 7)


def add_kernel(a, b, out):
    out[...] = a[...] + b[...]


def before_kernel(pieces, out):
    so_far = jnp.zeros(pieces.shape[1:], jnp.float32)
    for k in range(pieces.shape[0]):
        out[k] = so_far
        so_far = so_far + pieces[k]


def split_kernel(core, chips, own, got, mine, partners):
    @pl.when(core[0] == 0)
    def _():
        mine[...] = chips[...]
        partners[...] = chips[...] + own[...]

    @pl.when(core[0] != 0)
    def _():
        mine[...] = chips[...] + got[...]
        partners[...] = chips[...]


def half_potential(side, inner_held, rim_held, before, out, filled, done):
    half, cells = before.shape[:2]
    planes = planes_of((rim_held.at[0], inner_held, rim_held.at[1]), 2 * half)

    def fill(which):
        for j in range(half):
            y = which * half + j

            def body(i, carry, y=y, j=j):
                start = pl.multiple_of(i * BLOCK, BLOCK)
                for k in range(BLOCK):
                    x = start + k
                    filled[j, x] = planes[y][x] + jnp.broadcast_to(before[j, pl.ds(x, 1), :], (8, 128))
                return carry

            lax.fori_loop(0, cells // BLOCK, body, 0)
            pltpu.make_async_copy(filled.at[j], out.at[y], done.at[j]).start()
        for j in range(half):
            pltpu.make_async_copy(filled.at[j], out.at[which * half + j], done.at[j]).wait()

    @pl.when(side == 0)
    def _():
        fill(0)

    @pl.when(side != 0)
    def _():
        fill(1)


def own_half_kernel(core, low, high, inner_held, rim_held, before, end_in, out, end, filled, done, done_rims):
    copies = [
        pltpu.make_async_copy(low, end.at[0], done_rims.at[0]),
        pltpu.make_async_copy(high, end.at[end.shape[0] - 1], done_rims.at[1]),
    ]
    for copy in copies:
        copy.start()
    half_potential(core[0], inner_held, rim_held, before, out, filled, done)
    for copy in copies:
        copy.wait()


def other_half_kernel(core, inner_held, rim_held, before, out_in, out, filled, done):
    half_potential(1 - core[0], inner_held, rim_held, before, out, filled, done)


def sent(array, axis, by):
    size = lax.axis_size(axis)
    return lax.ppermute(array, axis, [(i, (i + by) % size) for i in range(size)])


def local(field_values, flow_y, flow_x, flow_z):
    core, field_values = lax.optimization_barrier((lax.axis_index("core").reshape(1), field_values))
    height, cells = field_values.shape[:2]
    flows = (flow_y, flow_x, flow_z)
    row, pair = shape(cells, 8, 128), shape(2, cells, 8, 128)
    inner = shape(height - 2, cells, 8, 128)
    whole = shape(*field_values.shape)
    edge, side = shape(height, cells, 128), shape(height, 8, 128)
    scalar = pl.BlockSpec(memory_space=pltpu.SMEM)

    def send_faces(field):
        first, last, left, right = call(
            functools.partial(faces_kernel, len(field), height), (edge, edge, side, side), *field
        )
        downs = sent(last, DOWN, 1), sent(first, DOWN, -1)
        sides = sent(right, "east", 1), sent(left, "east", -1)
        return (first, last), downs, sides

    def send_rim(low, high):
        return sent(high, "south", 1), sent(low, "south", -1)

    low, high = call(
        rows_kernel, (row, row), field_values, in_specs=[IN_HBM], scratch=[pltpu.SemaphoreType.DMA((2,))], vmem=48 << 20
    )
    slo, shi = send_rim(low, high)
    field = (field_values,)
    faces, downs, sides = send_faces(field)
    near = call(near_kernel, (edge, edge), flow_z)
    for step in range(1, STEPS + 1):
        parts = len(field)
        mid, *rims = call(
            functools.partial(inner_kernel, parts, height), (inner, row, row), *(*field, *flows), flops=1 << 23
        )
        (mid,) = call(
            functools.partial(mend_kernel, parts, height),
            (inner,),
            *(*field, *flows, *downs, *faces, *near, *sides, mid),
            alias={parts + 11: 0},
        )
        low, high = (
            call(
                functools.partial(rim_kernel, parts, height, top),
                (row,),
                *(*field, *flows, *downs, *faces, *near, *sides, beyond, rim),
                alias={parts + 12: 0},
            )[0]
            for top, beyond, rim in ((False, slo, rims[0]), (True, shi, rims[1]))
        )
        field = (low, mid, high)
        if step < STEPS:
            slo, shi = send_rim(low, high)
            faces, downs, sides = send_faces(field)
    chips = lax.axis_size("chip")
    scale = 1.0 / (8 * chips * 2)
    inner_held, end = call(
        functools.partial(inner_sums_kernel, scale),
        (inner, whole),
        mid,
        out_specs=[IN_VMEM, IN_HBM],
        scratch=[pltpu.SemaphoreType.DMA((1,))],
    )
    quarter = shape(height // 2, cells, 128)
    own, other, rim_held = call(
        functools.partial(rim_sums_kernel, scale),
        (quarter, quarter, pair),
        *(core, low, high, inner_held),
        in_specs=[scalar, *[IN_VMEM] * 3],
    )
    got = sent(other, "core", 1)
    (total,) = call(add_kernel, (quarter,), own, got)
    pieces = lax.all_to_all(total.reshape(chips, -1, 128), "chip", 0, 0, tiled=True)
    (pieces,) = call(before_kernel, (shape(*pieces.shape),), pieces)
    below = lax.all_to_all(pieces, "chip", 0, 0, tiled=True).reshape(total.shape)
    mine, partners = call(split_kernel, (quarter, quarter), core, below, own, got, in_specs=[scalar, *[IN_VMEM] * 3])
    theirs = sent(partners, "core", 1)
    rows_out = [pltpu.VMEM((height // 2, cells, 8, 128), jnp.float32), pltpu.SemaphoreType.DMA((height // 2,))]
    potential, end = call(
        own_half_kernel,
        (whole, whole),
        *(core, low, high, inner_held, rim_held, mine, end),
        in_specs=[scalar, *[IN_VMEM] * 5, IN_HBM],
        out_specs=[IN_HBM, IN_HBM],
        scratch=[*rows_out, pltpu.SemaphoreType.DMA((2,))],
        alias={6: 1},
    )
    (potential,) = call(
        other_half_kernel,
        (whole,),
        *(core, inner_held, rim_held, theirs, potential),
        in_specs=[scalar, *[IN_VMEM] * 3, IN_HBM],
        out_specs=[IN_HBM],
        scratch=rows_out,
        alias={4: 0},
    )
    return potential, end


def solution(mesh):
    finer = Mesh(
        mesh.devices.reshape(mesh.shape["south"], mesh.shape["east"], -1, 2), ("south", "east", "chip", "core")
    )
    spec = P("south", "east", DOWN, None)
    return jax.shard_map(local, mesh=finer, in_specs=(spec,) * 4, out_specs=(spec, spec), check_vma=False)
```

```python
import functools

import jax
import jax.numpy as jnp
from jax import lax
from jax.experimental import pallas as pl
from jax.experimental.pallas import tpu as pltpu
from jax.sharding import Mesh
from jax.sharding import PartitionSpec as P

STEPS = 4
RATE = 0.05
BLOCK = 8
GROUP = 4
VMEM = 5 << 20


DOWN = ("chip", "core")
IN_VMEM = pl.BlockSpec(memory_space=pltpu.VMEM)
IN_HBM = pl.BlockSpec(memory_space=pltpu.HBM)


def shape(*dims):
    return jax.ShapeDtypeStruct(dims, jnp.float32)


def call(kernel, outs, *args, flops=1 << 21, in_specs=None, out_specs=None, scratch=(), alias=None, vmem=VMEM):
    return pl.pallas_call(
        kernel,
        out_shape=outs,
        in_specs=in_specs or [IN_VMEM] * len(args),
        out_specs=out_specs or [IN_VMEM] * len(outs),
        scratch_shapes=scratch,
        input_output_aliases=alias or {},
        compiler_params=pltpu.CompilerParams(vmem_limit_bytes=vmem),
        cost_estimate=pl.CostEstimate(flops=flops, bytes_accessed=0, transcendentals=0),
    )(*args)


def advance(here, up, down, left, right, ahead, behind, fy, fx, fz):
    around = ((up + down) + (left + right)) + (ahead + behind)
    carried = (fy * (up - down) + fx * (right - left)) + fz * (ahead - behind)
    return ((1.0 - 6.0 * RATE) * here + RATE * around) - carried


def turned(here):
    return pltpu.roll(here, 7, 0), pltpu.roll(here, 1, 0)


def along_z(here, zlo, zhi, y, x):
    sublane = lax.broadcasted_iota(jnp.int32, (8, 128), 0)
    ahead, behind = turned(here)
    head = jnp.broadcast_to(zhi[y, pl.ds(x, 1), :], (8, 128))
    tail = jnp.broadcast_to(zlo[y, pl.ds(x, 1), :], (8, 128))
    return jnp.where(sublane == 7, head, ahead), jnp.where(sublane == 0, tail, behind)


def march(cells, column_at, cell):
    def run(start, first, last, left, mid):
        for k in range(first, last):
            right = column_at(start + k + 1)
            cell(start + k, left, mid, right)
            left, mid = mid, right
        return left, mid

    def body(i, carry):
        return run(pl.multiple_of(i * BLOCK, BLOCK), 0, BLOCK, *carry)

    carry = run(0, 1, BLOCK, column_at(0), column_at(1))
    carry = lax.fori_loop(1, cells // BLOCK - 1, body, carry)
    run(cells - BLOCK, 0, BLOCK - 1, *carry)


def reader(ref, *at):
    return lambda x: ref[(*at, x)]


def planes_of(refs, height):
    if len(refs) == 1:
        return [refs[0].at[y] for y in range(height)]
    low, inner, high = refs
    return [low, *(inner.at[y] for y in range(height - 2)), high]


def pack(plane, at):
    cells = plane.shape[0]
    return plane.reshape(cells * 8, 128)[pl.ds(at, cells, 8), :]


def inner_kernel(parts, height, scale, *refs):
    field, (fy, fx, fz) = refs[:parts], refs[parts : parts + 3]
    (out, low, high), sums = refs[parts + 3 : parts + 6], refs[parts + 6 :]
    cells = fy.shape[1]
    planes = [low, *(out.at[y] for y in range(height - 2)), high]
    nothing = lambda x: jnp.zeros((8, 128), jnp.float32)
    rows = [nothing, *(reader(plane) for plane in planes_of(field, height)), nothing]
    for start in range(0, height, GROUP):
        ys = list(range(start, min(start + GROUP, height)))

        def cell(x, left, mid, right, ys=ys):
            column = [rows[ys[0]](x), *mid, rows[ys[-1] + 2](x)]
            for g, y in enumerate(ys):
                planes[y][x] = advance(
                    mid[g], column[g + 2], column[g], left[g], right[g], *turned(mid[g]), fy[y, x], fx[y, x], fz[y, x]
                )

        march(cells, lambda x, ys=ys: [rows[y + 1](x) for y in ys], cell)
    for held in sums:
        for k in range(height - 2):

            def put(x, value, k=k):
                held[k, x] = value

            running_sums(scale, out.at[k], put)


def mend_kernel(parts, height, scale, *refs):
    field, (fy, fx, fz) = refs[:parts], refs[parts : parts + 3]
    (zlo, zhi), (first, last) = refs[parts + 3 : parts + 5], refs[parts + 5 : parts + 7]
    to_first, to_last = refs[parts + 7 : parts + 9]
    sides, outs = refs[parts + 9 : parts + 11], refs[parts + 12 :]
    out, held, lift = (outs[0], None, None) if scale is None else outs[1:]
    cells = fy.shape[1]
    rows = [reader(plane) for plane in planes_of(field, height)]
    for y in range(1, height - 1):
        flat = out.at[y - 1].reshape(cells * 8, 128)
        flat[pl.ds(0, cells, 8), :] += to_first[y] * (zlo[y] - last[y])
        flat[pl.ds(7, cells, 8), :] += to_last[y] * (zhi[y] - first[y])
        for x, left, right in (
            (0, sides[0][y], rows[y](1)),
            (cells - 1, rows[y](cells - 2), sides[1][y]),
        ):
            here = rows[y](x)
            out[y - 1, x] = advance(
                *(here, rows[y + 1](x), rows[y - 1](x), left, right),
                *along_z(here, zlo, zhi, y, x),
                *(fy[y, x], fx[y, x], fz[y, x]),
            )
        if held is not None:
            lift[y - 1] = (to_first[y] * (zlo[y] - last[y])) * scale
            sums = held.at[y - 1].reshape(cells * 8, 128)
            sums[pl.ds(7, cells, 8), :] += (to_last[y] * (zhi[y] - first[y])) * scale
            for x in (0, cells - 1):
                held[y - 1, x] = summed(out[y - 1, x] * scale)
                lift[y - 1, pl.ds(x, 1), :] = jnp.zeros((1, 128), jnp.float32)


def rim_kernel(parts, height, top, *refs):
    field, (fy, fx, fz) = refs[:parts], refs[parts : parts + 3]
    (zlo, zhi), (first, last) = refs[parts + 3 : parts + 5], refs[parts + 5 : parts + 7]
    to_first, to_last = refs[parts + 7 : parts + 9]
    sides, beyond, out = refs[parts + 9 : parts + 11], refs[parts + 11], refs[parts + 13]
    cells = fy.shape[1]
    rows = [reader(plane) for plane in planes_of(field, height)]
    y = height - 1 if top else 0

    def body(i, carry):
        start = pl.multiple_of(i * BLOCK, BLOCK)
        for k in range(BLOCK):
            x = start + k
            rate = RATE - fy[y, x] if top else RATE + fy[y, x]
            out[x] += rate * beyond[x]
        return carry

    lax.fori_loop(0, cells // BLOCK, body, 0)
    flat = out.reshape(cells * 8, 128)
    flat[pl.ds(0, cells, 8), :] += to_first[y] * (zlo[y] - last[y])
    flat[pl.ds(7, cells, 8), :] += to_last[y] * (zhi[y] - first[y])
    above, below = (reader(beyond), rows[y - 1]) if top else (rows[1], reader(beyond))
    for x, left, right in (
        (0, sides[0][y], rows[y](1)),
        (cells - 1, rows[y](cells - 2), sides[1][y]),
    ):
        here = rows[y](x)
        out[x] = advance(
            *(here, above(x), below(x), left, right),
            *along_z(here, zlo, zhi, y, x),
            *(fy[y, x], fx[y, x], fz[y, x]),
        )


def near_kernel(fz, to_first, to_last):
    for y in range(fz.shape[0]):
        to_first[y] = RATE + pack(fz.at[y], 0)
        to_last[y] = RATE - pack(fz.at[y], 7)


def rows_kernel(field, low, high, done):
    copies = [
        pltpu.make_async_copy(field.at[0], low, done.at[0]),
        pltpu.make_async_copy(field.at[field.shape[0] - 1], high, done.at[1]),
    ]
    for copy in copies:
        copy.start()
    for copy in copies:
        copy.wait()


def faces_kernel(parts, height, *refs):
    field, (first, last, left, right) = refs[:parts], refs[parts:]
    for y, plane in enumerate(planes_of(field, height)):
        first[y] = pack(plane, 0)
        last[y] = pack(plane, 7)
        left[y] = plane[0]
        right[y] = plane[plane.shape[0] - 1]


def summed(value):
    sublane = lax.broadcasted_iota(jnp.int32, (8, 128), 0)
    for reach in (1, 2, 4):
        value = value + jnp.where(sublane >= reach, pltpu.roll(value, reach, 0), 0.0)
    return value


def running_sums(scale, plane, put):
    def body(i, carry):
        start = pl.multiple_of(i * BLOCK, BLOCK)
        for k in range(BLOCK):
            put(start + k, summed(plane[start + k] * scale))
        return carry

    lax.fori_loop(0, plane.shape[0] // BLOCK, body, 0)


def write_kernel(inner, end, done):
    copy = pltpu.make_async_copy(inner, end.at[pl.ds(1, inner.shape[0])], done.at[0])
    copy.start()
    copy.wait()


def rim_sums_kernel(scale, core, low, high, inner_held, lift, own, other, held):
    half = own.shape[0]
    for k, plane in enumerate((low, high)):

        def put(x, value, k=k):
            held[k, x] = value

        running_sums(scale, plane, put)
    planes = planes_of((held.at[0], inner_held, held.at[1]), 2 * half)

    def total(y):
        over = pack(planes[y], 7)
        return over if y in (0, 2 * half - 1) else over + lift[y - 1]

    @pl.when(core[0] == 0)
    def _():
        for y in range(half):
            own[y] = total(y)
            other[y] = total(half + y)

    @pl.when(core[0] != 0)
    def _():
        for y in range(half):
            own[y] = total(half + y)
            other[y] = total(y)


def add_kernel(a, b, out):
    out[...] = a[...] + b[...]


def before_kernel(pieces, out):
    so_far = jnp.zeros(pieces.shape[1:], jnp.float32)
    for k in range(pieces.shape[0]):
        out[k] = so_far
        so_far = so_far + pieces[k]


def split_kernel(core, chips, own, got, mine, partners):
    @pl.when(core[0] == 0)
    def _():
        mine[...] = chips[...]
        partners[...] = chips[...] + own[...]

    @pl.when(core[0] != 0)
    def _():
        mine[...] = chips[...] + got[...]
        partners[...] = chips[...]


def half_potential(side, inner_held, rim_held, lift, before, out, filled, base, done):
    half, cells = before.shape[:2]
    planes = planes_of((rim_held.at[0], inner_held, rim_held.at[1]), 2 * half)

    def fill(which):
        for j in range(half):
            y = which * half + j
            base[j] = before[j] if y in (0, 2 * half - 1) else before[j] + lift[y - 1]

            def body(i, carry, y=y, j=j):
                start = pl.multiple_of(i * BLOCK, BLOCK)
                for k in range(BLOCK):
                    x = start + k
                    filled[j, x] = planes[y][x] + jnp.broadcast_to(base[j, pl.ds(x, 1), :], (8, 128))
                return carry

            lax.fori_loop(0, cells // BLOCK, body, 0)
            pltpu.make_async_copy(filled.at[j], out.at[y], done.at[j]).start()
        for j in range(half):
            pltpu.make_async_copy(filled.at[j], out.at[which * half + j], done.at[j]).wait()

    @pl.when(side == 0)
    def _():
        fill(0)

    @pl.when(side != 0)
    def _():
        fill(1)


def own_half_kernel(core, low, high, inner_held, rim_held, lift, before, end_in, out, end, filled, base, done, done_rims):
    copies = [
        pltpu.make_async_copy(low, end.at[0], done_rims.at[0]),
        pltpu.make_async_copy(high, end.at[end.shape[0] - 1], done_rims.at[1]),
    ]
    for copy in copies:
        copy.start()
    half_potential(core[0], inner_held, rim_held, lift, before, out, filled, base, done)
    for copy in copies:
        copy.wait()


def other_half_kernel(core, inner_held, rim_held, lift, before, out_in, out, filled, base, done):
    half_potential(1 - core[0], inner_held, rim_held, lift, before, out, filled, base, done)


def sent(array, axis, by):
    size = lax.axis_size(axis)
    return lax.ppermute(array, axis, [(i, (i + by) % size) for i in range(size)])


def local(field_values, flow_y, flow_x, flow_z):
    core, field_values = lax.optimization_barrier((lax.axis_index("core").reshape(1), field_values))
    height, cells = field_values.shape[:2]
    flows = (flow_y, flow_x, flow_z)
    row, pair = shape(cells, 8, 128), shape(2, cells, 8, 128)
    inner = shape(height - 2, cells, 8, 128)
    whole = shape(*field_values.shape)
    edge, side = shape(height, cells, 128), shape(height, 8, 128)
    scalar = pl.BlockSpec(memory_space=pltpu.SMEM)
    chips = lax.axis_size("chip")
    scale = 1.0 / (8 * chips * 2)

    def send_faces(field):
        first, last, left, right = call(
            functools.partial(faces_kernel, len(field), height), (edge, edge, side, side), *field
        )
        downs = sent(last, DOWN, 1), sent(first, DOWN, -1)
        sides = sent(right, "east", 1), sent(left, "east", -1)
        return (first, last), downs, sides

    def send_rim(low, high):
        return sent(high, "south", 1), sent(low, "south", -1)

    low, high = call(
        rows_kernel, (row, row), field_values, in_specs=[IN_HBM], scratch=[pltpu.SemaphoreType.DMA((2,))], vmem=48 << 20
    )
    slo, shi = send_rim(low, high)
    field = (field_values,)
    faces, downs, sides = send_faces(field)
    near = call(near_kernel, (edge, edge), flow_z)
    for step in range(1, STEPS + 1):
        parts = len(field)
        last_scale = scale if step == STEPS else None
        sums = () if last_scale is None else (inner,)
        mid, low_part, high_part, *held = call(
            functools.partial(inner_kernel, parts, height, scale),
            (inner, row, row, *sums),
            *(*field, *flows),
            flops=1 << 23,
        )
        mid, *held = call(
            functools.partial(mend_kernel, parts, height, last_scale),
            (inner, inner, shape(height - 2, cells, 128)) if held else (inner,),
            *(*field, *flows, *downs, *faces, *near, *sides, mid, *held),
            alias={parts + 11: 0, parts + 12: 1} if held else {parts + 11: 0},
        )
        low, high = (
            call(
                functools.partial(rim_kernel, parts, height, top),
                (row,),
                *(*field, *flows, *downs, *faces, *near, *sides, beyond, rim),
                alias={parts + 12: 0},
            )[0]
            for top, beyond, rim in ((False, slo, low_part), (True, shi, high_part))
        )
        field = (low, mid, high)
        if step < STEPS:
            slo, shi = send_rim(low, high)
            faces, downs, sides = send_faces(field)
    inner_held, lift = held
    quarter = shape(height // 2, cells, 128)
    own, other, rim_held = call(
        functools.partial(rim_sums_kernel, scale),
        (quarter, quarter, pair),
        *(core, low, high, inner_held, lift),
        in_specs=[scalar, *[IN_VMEM] * 4],
    )
    got = sent(other, "core", 1)
    (end,) = call(write_kernel, (whole,), mid, out_specs=[IN_HBM], scratch=[pltpu.SemaphoreType.DMA((1,))])
    (total,) = call(add_kernel, (quarter,), own, got)
    pieces = lax.all_to_all(total.reshape(chips, -1, 128), "chip", 0, 0, tiled=True)
    (pieces,) = call(before_kernel, (shape(*pieces.shape),), pieces)
    below = lax.all_to_all(pieces, "chip", 0, 0, tiled=True).reshape(total.shape)
    mine, partners = call(split_kernel, (quarter, quarter), core, below, own, got, in_specs=[scalar, *[IN_VMEM] * 3])
    theirs = sent(partners, "core", 1)
    rows_out = [pltpu.VMEM((height // 2, cells, 8, 128), jnp.float32), pltpu.VMEM(quarter.shape, jnp.float32), pltpu.SemaphoreType.DMA((height // 2,))]
    potential, end = call(
        own_half_kernel,
        (whole, whole),
        *(core, low, high, inner_held, rim_held, lift, mine, end),
        in_specs=[scalar, *[IN_VMEM] * 6, IN_HBM],
        out_specs=[IN_HBM, IN_HBM],
        scratch=[*rows_out, pltpu.SemaphoreType.DMA((2,))],
        alias={7: 1},
    )
    (potential,) = call(
        other_half_kernel,
        (whole,),
        *(core, inner_held, rim_held, lift, theirs, potential),
        in_specs=[scalar, *[IN_VMEM] * 4, IN_HBM],
        out_specs=[IN_HBM],
        scratch=rows_out,
        alias={5: 0},
    )
    return potential, end


def solution(mesh):
    finer = Mesh(
        mesh.devices.reshape(mesh.shape["south"], mesh.shape["east"], -1, 2), ("south", "east", "chip", "core")
    )
    spec = P("south", "east", DOWN, None)
    return jax.shard_map(local, mesh=finer, in_specs=(spec,) * 4, out_specs=(spec, spec), check_vma=False)
```
